32 devices in a mesh: section: 4 (over z), dp: 2 (over y), mp: 4 (over x, core).
Axes of the slice: x: 2, y: 2, z: 4, core: 2. Of those that a mesh axis runs over, the one named last changes fastest.
Arguments:
- text: bfloat16 [4, 1024, 4096], P('section', ('dp', 'mp')), may hold values from -6 to 6
- patches: bfloat16 [4096, 1024], P(('section', 'dp')), may hold values from -6 to 6
- segments: int32 [4, 2, 512], P('section', 'dp'), may hold values from 0 to 3, never falling along the last dimension, each value on 1 to 256 neighbouring positions
- loss_mask: int32 [4, 1024], P('section', ('dp', 'mp')), may hold values from 0 to 1, as said below
- tile_batch: int32 [2, 8], P('dp'), may hold values from 0 to 3, as said below
- tile_offset: int32 [2, 8], P('dp'), may hold values from 0 to 448, as said below
- attn_gain: float32 [4, 4096], P('section'), may hold values from 0.5 to 2
- w_query: bfloat16 [4, 4096, 2048], P('section', None, 'mp'), may hold values from -0.09375 to 0.09375
- w_kv: bfloat16 [4, 2, 4096, 512], P('section', None, None, 'mp'), may hold values from -0.09375 to 0.09375
- w_out: bfloat16 [4, 2048, 4096], P('section', 'mp'), may hold values from -0.125 to 0.125
- vis_gain: float32 [2, 1024], replicated, may hold values from 0.5 to 2
- vis_bias: float32 [2, 1024], replicated, may hold values from -3 to 3
- v_qkv: bfloat16 [3, 1024, 1024], P(None, ('section', 'dp'), 'mp'), may hold values from -0.1875 to 0.1875
- v_out: bfloat16 [1024, 1024], P('mp', ('section', 'dp')), may hold values from -0.1875 to 0.1875
- v_up: bfloat16 [1024, 4096], P(('section', 'dp'), 'mp'), may hold values from -0.1875 to 0.1875
- v_down: bfloat16 [4096, 1024], P('mp', ('section', 'dp')), may hold values from -0.09375 to 0.09375
- v_proj: bfloat16 [4096, 4096], P(('section', 'dp'), 'mp'), may hold values from -0.09375 to 0.09375
Outputs:
- hidden: bfloat16 [4, 1024, 4096], P('section', ('dp', 'mp'))
- token_weight: float32 [4, 1024], P('section', ('dp', 'mp'))
The draws below stay inside these ranges and needn't reach their ends.
Inputs may be any that keep to these rules, and one draw needn't show every extreme that they name: `tile_batch`: in every data-parallel index, the 2 tiles of each section index go 1 to each of two different micro-batches; one micro-batch receives 1 tiles from every section index. `tile_offset`: offsets are multiples of 64; the runs of one sequence never intersect. `loss_mask`: the first position of every sequence is a one.
All inputs are finite; a program needn't handle non-finite values.
Results may differ from the reference program's by a relative error of at most 0.025.
Values may be sent and summed in bfloat16 or wider, within the bound.
A program may use at most 192 MiB of HBM per device.

```python
import math
import jax
import jax.numpy as jnp
import numpy as np
from jax import lax

D = 4096
QH = 16
KVH = 4
HD = 128
VD = 1024
VH = 16
VHD = 64
VFF = 4096
GRID = 16
PATCH = 256
POOL = 64
L = 512
TILES_G = 2
CAP = 1
MICRO = 4
TILES = 16
N_SECTION = 4
N_DP = 2
N_MP = 4


def tile_plan(key):
    base_key = jax.random.fold_in(key, 7)
    target_key, second_key, order_key, slot_key = jax.random.split(base_key, 4)
    tile_count = N_SECTION * TILES_G
    target = jax.random.randint(target_key, (N_DP, 1), 0, MICRO)
    moved = jax.random.randint(second_key, (N_DP, N_SECTION), 1, MICRO)
    second = jnp.mod(target + moved, MICRO)
    orders = jax.vmap(lambda item_key: jax.random.permutation(item_key, TILES_G))(jax.random.split(order_key, N_DP * N_SECTION))
    orders = orders.reshape(N_DP, N_SECTION, TILES_G)
    batches = jnp.where(orders < CAP, target[:, :, None], second[:, :, None]).reshape(N_DP, tile_count)
    tile_ids = jnp.arange(tile_count, dtype=jnp.int32)
    earlier = tile_ids[None, :] < tile_ids[:, None]
    same = batches[:, :, None] == batches[:, None, :]
    ranks = jnp.sum((same & earlier[None, :, :]).astype(jnp.int32), axis=2)
    slot_total = L // POOL
    slot_perm = jax.vmap(lambda item_key: jax.random.permutation(item_key, slot_total))(jax.random.split(slot_key, N_DP * MICRO))
    slot_perm = slot_perm.reshape(N_DP, MICRO * slot_total)
    offsets = POOL * jnp.take_along_axis(slot_perm, batches * slot_total + ranks, axis=1)
    return (batches.astype(jnp.int32), offsets.astype(jnp.int32))


def draw_tile_batch(key, part):
    batches, offsets = tile_plan(key)
    return batches


def draw_tile_offset(key, part):
    batches, offsets = tile_plan(key)
    return offsets


def draw_loss_mask(key, part):
    seq_count = MICRO * N_DP
    seq_index = jnp.arange(seq_count, dtype=jnp.int32)
    threshold = 250 + 500 * seq_index // max(seq_count - 1, 1)
    rolls = jax.random.randint(jax.random.fold_in(key, 5), (seq_count, L), 0, 1000)
    marked = (rolls < threshold[:, None]).astype(jnp.int32)
    leading = (jnp.arange(L) == 0).astype(jnp.int32)
    marked = jnp.maximum(marked, leading[None, :])
    return marked.reshape(MICRO, N_DP * L)


def gain_values(key, shape):
    return jax.random.uniform(key, shape, jnp.float32, 0.5, 1.5)


def draw_attn_gain(key, part):
    return gain_values(jax.random.fold_in(key, 3), (N_SECTION, D))


def draw_vis_gain(key, part):
    return gain_values(jax.random.fold_in(key, 4), (2, VD))


def shard_levels(stream_key, extent, pieces, low, high):
    level, own = 1.0, jax.random.fold_in(stream_key, 6)
    for axis_at, shards_of in pieces:
        heights = jnp.exp(jax.random.uniform(jax.random.fold_in(own, axis_at), (shards_of,), jnp.float32, low / len(pieces), high / len(pieces)))
        level = level * jnp.repeat(heights, extent[axis_at] // shards_of).reshape([-1 if axis == axis_at else 1 for axis in range(len(extent))])
    return level


def split_up(number_of, total, bound, slope):
    loads = [(1 << 20) // math.isqrt(grade ** slope) + 1 for grade in range(2, number_of + 1)]
    surplus, given = total - bound - (number_of - 1), [1] * (number_of - 1)
    while surplus > 0:
        free = [i for i in range(number_of - 1) if given[i] < bound]
        pool, remaining = sum([loads[i] for i in free]), surplus
        for i in free:
            extra = min(bound - given[i], max(1, remaining * loads[i] // pool), surplus)
            given[i] = given[i] + extra
            surplus = surplus - extra
    return np.array([bound] + given)


def uneven(rng, count, total, reach, slope):
    if count == 2:
        one = jax.random.randint(rng, (), max(1, total - reach), min(reach, total - 1) + 1)
        return jnp.stack([one, total - one])
    sizes = jnp.asarray(split_up(count, total, reach, slope), jnp.int32)
    twos = (count - 1) // 2
    source_of, sink = sizes[1:1 + 2 * twos:2], sizes[2:2 + 2 * twos:2]
    margin = jnp.minimum(source_of - 1, reach - sink)
    shifted = jax.random.randint(jax.random.fold_in(rng, 1), (twos,), 0, 1 << 20) % (margin + 1)
    sizes = sizes.at[1:1 + 2 * twos:2].set(source_of - shifted).at[2:2 + 2 * twos:2].set(sink + shifted)
    return sizes[jax.random.permutation(jax.random.fold_in(rng, 2), count)]


def normal_values(stream_key, shape, scale, bound, pieces=(), kind=jnp.bfloat16):
    values = jax.random.normal(stream_key, shape, jnp.float32) * scale
    if len(pieces) > 0:
        values = shard_levels(stream_key, shape, pieces, -0.22, 0.18) * values
    return jnp.clip(values, min=-bound, max=bound).astype(kind)


def setup_inputs(seed: int = 0) -> dict:
    key_list = jax.random.split(jax.random.key(seed), 18)
    return {
        "text": normal_values(key_list[0], (MICRO, N_DP * L, D), 1.0, 6.0, ((0, 4), (1, 8))),
        "patches": normal_values(key_list[1], (TILES * PATCH, VD), 1.0, 6.0, ((0, 8),)),
        "segments": jax.vmap(lambda own: jnp.searchsorted(jnp.cumsum(uneven(own, 4, L, L // 2, 2)), jnp.arange(L), side="right"))(jax.random.split(key_list[2], MICRO * N_DP)).reshape((MICRO, N_DP, L)).astype(jnp.int32),
        "loss_mask": draw_loss_mask(jax.random.fold_in(key_list[17], 71), 0),
        "tile_batch": draw_tile_batch(jax.random.fold_in(key_list[17], 71), 0),
        "tile_offset": draw_tile_offset(jax.random.fold_in(key_list[17], 71), 0),
        "attn_gain": draw_attn_gain(jax.random.fold_in(key_list[17], 71), 0),
        "w_query": normal_values(key_list[7], (N_SECTION, D, QH * HD), D ** -0.5, 0.09375, ((0, 4), (2, 4))),
        "w_kv": normal_values(key_list[8], (N_SECTION, 2, D, KVH * HD), D ** -0.5, 0.09375, ((0, 4), (3, 4))),
        "w_out": normal_values(key_list[9], (N_SECTION, QH * HD, D), (QH * HD) ** -0.5, 0.125, ((0, 4), (1, 4))),
        "vis_gain": draw_vis_gain(jax.random.fold_in(key_list[17], 71), 0),
        "vis_bias": normal_values(key_list[11], (2, VD), 0.5, 3.0, (), jnp.float32),
        "v_qkv": normal_values(key_list[12], (3, VD, VD), VD ** -0.5, 0.1875, ((1, 8), (2, 4))),
        "v_out": normal_values(key_list[13], (VD, VD), VD ** -0.5, 0.1875, ((0, 4), (1, 8))),
        "v_up": normal_values(key_list[14], (VD, VFF), VD ** -0.5, 0.1875, ((0, 8), (1, 4))),
        "v_down": normal_values(key_list[15], (VFF, VD), VFF ** -0.5, 0.09375, ((0, 4), (1, 8))),
        "v_proj": normal_values(key_list[16], (4 * VD, D), (4 * VD) ** -0.5, 0.09375, ((0, 8), (1, 4))),
    }


EPS = 1e-05
ROPE_BASE = 500000.0
BLOCKED = -1e+30

def layer_norm(values, gain, bias):
    wide = values.astype(jnp.float32)
    center = wide - lax.optimization_barrier(jnp.mean(wide, axis=-1, keepdims=True))
    spread = lax.optimization_barrier(jnp.mean(center * center, axis=-1, keepdims=True))
    return (center * lax.rsqrt(spread + EPS) * gain + bias).astype(jnp.bfloat16)

def rms_norm(values, gain):
    wide = values.astype(jnp.float32)
    power = lax.optimization_barrier(jnp.mean(wide * wide, axis=-1, keepdims=True))
    return (wide * lax.rsqrt(power + EPS) * gain).astype(jnp.bfloat16)

def rotate(values, positions):
    half_width = values.shape[-1] // 2
    freqs = ROPE_BASE ** (-2.0 * jnp.arange(half_width, dtype=jnp.float32) / values.shape[-1])
    angles = positions.astype(jnp.float32)[:, None] * freqs[None, :]
    cosine = jnp.cos(angles)[:, None, :]
    sinus_part = jnp.sin(angles)[:, None, :]
    first_half = values[..., :half_width]
    second_half = values[..., half_width:]
    return jnp.concatenate([first_half * cosine - second_half * sinus_part, second_half * cosine + first_half * sinus_part], axis=-1)

def split_sum(left, right):
    row_count = left.shape[0]
    block_width = left.shape[1] // N_MP
    left_blocks = left.reshape(row_count, N_MP, block_width).astype(jnp.float32)
    right_blocks = right.reshape(N_MP, block_width, right.shape[1]).astype(jnp.float32)
    partials = jnp.einsum('rgk,gkn->grn', left_blocks, right_blocks)
    rounded = lax.optimization_barrier(partials.astype(jnp.bfloat16))
    return lax.optimization_barrier(jnp.sum(rounded.astype(jnp.float32), axis=0))

def pixel_shuffle(states):
    tile_count = states.shape[0] // PATCH
    side_half = GRID // 2
    width = states.shape[1]
    arranged = states.reshape(tile_count, side_half, 2, side_half, 2, width)
    return arranged.transpose(0, 1, 3, 2, 4, 5).reshape(tile_count * side_half * side_half, 4 * width)

def encode_group(block, vis_gain, vis_bias, v_qkv, v_out, v_up, v_down, v_proj):
    tile_count = block.shape[0] // PATCH
    normed = layer_norm(block, vis_gain[0], vis_bias[0])
    projected = [jnp.dot(normed, v_qkv[index], preferred_element_type=jnp.float32).astype(jnp.bfloat16).reshape(tile_count, PATCH, VH, VHD) for index in range(3)]
    scores = jnp.einsum('tqhd,tkhd->thqk', projected[0].astype(jnp.float32), projected[1].astype(jnp.float32)) * VHD ** (-0.5)
    probs = jax.nn.softmax(scores, axis=-1).astype(jnp.bfloat16)
    mixed = jnp.einsum('thqk,tkhd->tqhd', probs.astype(jnp.float32), projected[2].astype(jnp.float32)).astype(jnp.bfloat16).reshape(tile_count * PATCH, VD)
    residual = (block.astype(jnp.float32) + split_sum(mixed, v_out)).astype(jnp.bfloat16)
    normed_two = layer_norm(residual, vis_gain[1], vis_bias[1])
    inner = jax.nn.gelu(jnp.dot(normed_two, v_up, preferred_element_type=jnp.float32), approximate=False).astype(jnp.bfloat16)
    states = (residual.astype(jnp.float32) + split_sum(inner, v_down)).astype(jnp.bfloat16)
    return jnp.dot(pixel_shuffle(states), v_proj, preferred_element_type=jnp.float32).astype(jnp.bfloat16)

def decoder_layer(state, segment_ids, gain, w_query, w_kv, w_out):
    length = state.shape[0]
    positions = jnp.arange(length, dtype=jnp.int32)
    normed = rms_norm(state, gain)
    query = rotate(jnp.dot(normed, w_query, preferred_element_type=jnp.float32).reshape(length, QH, HD), positions).astype(jnp.bfloat16)
    keyed = rotate(jnp.dot(normed, w_kv[0], preferred_element_type=jnp.float32).reshape(length, KVH, HD), positions).astype(jnp.bfloat16)
    valued = jnp.dot(normed, w_kv[1], preferred_element_type=jnp.float32).astype(jnp.bfloat16).reshape(length, KVH, HD)
    grouped = query.reshape(length, KVH, QH // KVH, HD).astype(jnp.float32)
    scores = jnp.einsum('qkgd,skd->kgqs', grouped, keyed.astype(jnp.float32)) * HD ** (-0.5)
    allowed = (segment_ids[:, None] == segment_ids[None, :]) & (positions[None, :] <= positions[:, None])
    scores = jnp.where(allowed, scores, BLOCKED)
    probs = jax.nn.softmax(scores, axis=-1).astype(jnp.bfloat16)
    mixed = jnp.einsum('kgqs,skd->qkgd', probs.astype(jnp.float32), valued.astype(jnp.float32)).astype(jnp.bfloat16).reshape(length, QH * HD)
    return (state.astype(jnp.float32) + split_sum(mixed, w_out)).astype(jnp.bfloat16)

def reference(text, patches, segments, loss_mask, tile_batch, tile_offset, attn_gain, w_query, w_kv, w_out, vis_gain, vis_bias, v_qkv, v_out, v_up, v_down, v_proj):
    group_count = N_SECTION * N_DP
    grouped = patches.reshape(group_count, TILES_G * PATCH, VD)
    embedded = lax.map(lambda block: encode_group(block, vis_gain, vis_bias, v_qkv, v_out, v_up, v_down, v_proj), grouped)
    per_tile = embedded.reshape(N_SECTION, N_DP, TILES_G, POOL, D).transpose(1, 0, 2, 3, 4).reshape(N_DP, N_SECTION * TILES_G, POOL, D)
    states = text.reshape(MICRO, N_DP, L, D)
    places = tile_offset[:, :, None] + jnp.arange(POOL, dtype=jnp.int32)[None, None, :]
    dp_ids = jnp.broadcast_to(jnp.arange(N_DP, dtype=jnp.int32)[:, None, None], places.shape)
    micro_ids = jnp.broadcast_to(tile_batch[:, :, None], places.shape)
    states = states.at[micro_ids, dp_ids, places].set(per_tile)
    flat_states = states.reshape(MICRO * N_DP, L, D)
    flat_segments = segments.reshape(MICRO * N_DP, L)

    def run_sequence(pair):
        state, segment_ids = pair
        for layer_index in range(N_SECTION):
            state = decoder_layer(state, segment_ids, attn_gain[layer_index], w_query[layer_index], w_kv[layer_index], w_out[layer_index])
        return state
    hidden = lax.map(run_sequence, (flat_states, flat_segments)).reshape(MICRO, N_DP * L, D)
    weights = loss_mask.astype(jnp.float32)
    token_weight = weights * (MICRO * N_DP * L) / jnp.sum(weights)
    return (hidden, token_weight)
```

```python
import jax
import jax.numpy as jnp
from jax import lax
from jax.sharding import PartitionSpec as P

HD = 128
VHD = 64
GRID = 16
PATCH = 256
POOL = 64


EPS = 1e-05
ROPE_BASE = 500000.0
BLOCKED = -1e30


def layer_norm(values, gain, bias):
    wide = values.astype(jnp.float32)
    center = wide - jnp.mean(wide, axis=-1, keepdims=True)
    spread = jnp.mean(center * center, axis=-1, keepdims=True)
    return (center * lax.rsqrt(spread + EPS) * gain + bias).astype(jnp.bfloat16)


def rms_norm(values, gain):
    wide = values.astype(jnp.float32)
    power = jnp.mean(wide * wide, axis=-1, keepdims=True)
    return (wide * lax.rsqrt(power + EPS) * gain).astype(jnp.bfloat16)


def mirrored(value, bit):
    count = lax.axis_size("mp")
    return lax.ppermute(value, "mp", [(at, at ^ bit) for at in range(count)])


def slot_order(count):
    order = [0]
    bit = count // 2
    while bit >= 1:
        order = order + [slot | bit for slot in order]
        bit //= 2
    return order


def gather_slots(piece):
    count = lax.axis_size("mp")
    held = {0: piece}
    bit = count // 2
    while bit >= 1:
        for slot in list(held):
            held[slot | bit] = mirrored(held[slot], bit)
        bit //= 2
    return [held[slot] for slot in slot_order(count)]


def scatter_slots(partial_value):
    count = lax.axis_size("mp")
    current = partial_value
    bit = 1
    while bit < count:
        half = current.shape[0] // 2
        arrived = mirrored(current[half:].astype(jnp.bfloat16), bit)
        current = current[:half].astype(jnp.float32) + arrived.astype(jnp.float32)
        bit *= 2
    return current


def own_slots(values, part_at):
    count = lax.axis_size("mp")
    rows = values.shape[0] // count
    return jnp.concatenate(
        [
            lax.dynamic_slice_in_dim(values, (part_at ^ slot) * rows, rows, 0)
            for slot in slot_order(count)
        ],
        axis=0,
    )


def encode_tiles(patches, vis_gain, vis_bias, qkv_full, out_full, up_full, down_full, part_at):
    tile_count = patches.shape[0] // PATCH
    local_width = qkv_full.shape[1] // 3
    head_count = local_width // VHD
    normed = layer_norm(patches, vis_gain[0], vis_bias[0])
    projected = [
        jnp.dot(
            normed,
            qkv_full[:, index * local_width : (index + 1) * local_width],
            preferred_element_type=jnp.float32,
        )
        .astype(jnp.bfloat16)
        .reshape(tile_count, PATCH, head_count, VHD)
        for index in range(3)
    ]
    scores = jnp.einsum(
        "tqhd,tkhd->thqk", projected[0], projected[1], preferred_element_type=jnp.float32
    ) * VHD ** (-0.5)
    probs = jax.nn.softmax(scores, axis=-1).astype(jnp.bfloat16)
    mixed = (
        jnp.einsum("thqk,tkhd->tqhd", probs, projected[2], preferred_element_type=jnp.float32)
        .astype(jnp.bfloat16)
        .reshape(tile_count * PATCH, local_width)
    )
    mixed = own_slots(mixed, part_at)
    attended = scatter_slots(
        jnp.dot(mixed, out_full, preferred_element_type=jnp.float32).astype(jnp.bfloat16)
    )
    rows = attended.shape[0]
    own = lax.dynamic_slice_in_dim(patches, part_at * rows, rows, 0)
    residual = (own.astype(jnp.float32) + attended).astype(jnp.bfloat16)
    normed_two = jnp.concatenate(
        gather_slots(layer_norm(residual, vis_gain[1], vis_bias[1])), axis=0
    )
    inner = jax.nn.gelu(
        jnp.dot(normed_two, up_full, preferred_element_type=jnp.float32), approximate=False
    ).astype(jnp.bfloat16)
    fed = scatter_slots(
        jnp.dot(inner, down_full, preferred_element_type=jnp.float32).astype(jnp.bfloat16)
    )
    states = (residual.astype(jnp.float32) + fed).astype(jnp.bfloat16)
    width = states.shape[1]
    arranged = states.reshape(rows // (2 * GRID), 2, GRID // 2, 2, width)
    return arranged.transpose(0, 2, 1, 3, 4).reshape(rows // 4, 4 * width)


def rotary(joined, cosine, sinus):
    half = HD // 2
    outs = []
    for at in range(0, joined.shape[1], HD):
        first = joined[:, at : at + half]
        second = joined[:, at + half : at + HD]
        outs.append(first * cosine - second * sinus)
        outs.append(second * cosine + first * sinus)
    return jnp.concatenate(outs, axis=1)


CHUNKS = 2


def decoder_layer(chunks, seg_row, positions, cosine, sinus, gain, w_joined, w_out, query_width):
    pair_width = (w_joined.shape[1] - query_width) // 2
    rotated = query_width + pair_width
    pair_heads = pair_width // HD
    group_size = query_width // pair_width
    joined = []
    rows_each = chunks[0].shape[0] * lax.axis_size("mp")
    for at, chunk in enumerate(chunks):
        rows = jnp.concatenate(gather_slots(rms_norm(chunk, gain)), axis=0)
        made = jnp.dot(rows, w_joined, preferred_element_type=jnp.float32)
        part = slice(at * rows_each, (at + 1) * rows_each)
        joined.append(
            jnp.concatenate(
                [rotary(made[:, :rotated], cosine[part], sinus[part]), made[:, rotated:]], axis=1
            ).astype(jnp.bfloat16)
        )
    joined = jnp.concatenate(joined, axis=0)
    length = joined.shape[0]
    query = joined[:, :query_width].reshape(length, pair_heads, group_size, HD)
    keyed = joined[:, query_width:rotated].reshape(length, pair_heads, HD)
    valued = joined[:, rotated:].reshape(length, pair_heads, HD)
    scores = jnp.einsum(
        "qkgd,skd->kgqs", query, keyed, preferred_element_type=jnp.float32
    ) * HD ** (-0.5)
    allowed = (seg_row[:, None] == seg_row[None, :]) & (
        positions[None, :] <= positions[:, None]
    )
    scores = jnp.where(allowed, scores, BLOCKED)
    probs = jax.nn.softmax(scores, axis=-1).astype(jnp.bfloat16)
    mixed = (
        jnp.einsum("kgqs,skd->qkgd", probs, valued, preferred_element_type=jnp.float32)
        .astype(jnp.bfloat16)
        .reshape(length, query_width)
    )
    outs = []
    for at, chunk in enumerate(chunks):
        made = jnp.dot(
            mixed[at * rows_each : (at + 1) * rows_each], w_out, preferred_element_type=jnp.float32
        ).astype(jnp.bfloat16)
        outs.append((chunk.astype(jnp.float32) + scatter_slots(made)).astype(jnp.bfloat16))
    return outs


def shards(
    text,
    patches,
    segments,
    loss_mask,
    tile_batch,
    tile_offset,
    attn_gain,
    w_query,
    w_kv,
    w_out,
    vis_gain,
    vis_bias,
    v_qkv,
    v_out,
    v_up,
    v_down,
    v_proj,
):
    sections = lax.axis_size("section")
    replicas = lax.axis_size("dp")
    parts = lax.axis_size("mp")
    section_at = lax.axis_index("section")
    part_at = lax.axis_index("mp")
    slots = slot_order(parts)
    groups = ("section", "dp")
    qkv_full = lax.all_gather(
        jnp.concatenate([v_qkv[0], v_qkv[1], v_qkv[2]], axis=1), groups, axis=0, tiled=True
    )
    backs = lax.all_gather(
        jnp.concatenate([v_out, v_down], axis=0), groups, axis=1, tiled=True
    )
    up_full = lax.all_gather(v_up, groups, axis=0, tiled=True)
    out_full = backs[: v_out.shape[0]]
    down_full = backs[v_out.shape[0] :]
    length = segments.shape[2]
    totals = lax.psum(lax.psum(lax.psum(jnp.sum(loss_mask), "mp"), "dp"), "section")
    seg_all = lax.all_gather(segments[0, 0], "section", axis=0)
    patches, totals, seg_all = lax.optimization_barrier((patches, totals, seg_all))
    scaling = float(sections * replicas * length)
    token_weight = loss_mask.astype(jnp.float32) * scaling / totals.astype(jnp.float32)

    pooled = encode_tiles(
        patches, vis_gain, vis_bias, qkv_full, out_full, up_full, down_full, part_at
    )
    own_rows = pooled.shape[0]
    group_count = sections * replicas
    depth = v_proj.shape[0]
    cut = pooled.reshape(own_rows, group_count, depth).transpose(1, 0, 2)
    dealt = lax.all_to_all(cut, groups, split_axis=0, concat_axis=0, tiled=True)
    stacked = jnp.stack(gather_slots(dealt), axis=1)
    width = v_proj.shape[1]
    projected = jnp.dot(
        stacked.reshape(group_count * parts * own_rows, depth),
        v_proj,
        preferred_element_type=jnp.float32,
    ).astype(jnp.bfloat16)
    image_own = lax.psum_scatter(projected, groups, scatter_dimension=0, tiled=True)
    image_all = lax.all_gather(image_own, "section", axis=0, tiled=True)
    batch_all = tile_batch[0]
    offset_all = tile_offset[0]
    tiles_here = own_rows * parts // POOL
    token_at = jnp.concatenate(
        [(part_at ^ slot) * own_rows + jnp.arange(own_rows, dtype=jnp.int32) for slot in slots]
    )
    tile_at = (
        jnp.arange(sections, dtype=jnp.int32)[:, None] * tiles_here + (token_at // POOL)[None, :]
    ).reshape(-1)
    within = jnp.tile(token_at % POOL, sections)
    tile_ids = jnp.arange(batch_all.shape[0], dtype=jnp.int32)
    pick = (tile_at[:, None] == tile_ids[None, :]).astype(jnp.int32)
    row_batch = jnp.sum(pick * batch_all[None, :], axis=1)
    row_place = jnp.sum(pick * offset_all[None, :], axis=1) + within
    places = jnp.arange(length, dtype=jnp.int32)
    picker = (
        (row_batch == section_at)[None, :] & (places[:, None] == row_place[None, :])
    ).astype(jnp.bfloat16)
    image_cols = jnp.dot(picker, image_all, preferred_element_type=jnp.float32).astype(
        jnp.bfloat16
    )
    image_rows = lax.all_to_all(image_cols, "mp", split_axis=0, concat_axis=1, tiled=True)
    shard_rows = image_rows.shape[0]
    own_places = part_at * shard_rows + jnp.arange(shard_rows, dtype=jnp.int32)
    covered = jnp.any(
        (batch_all[None, :] == section_at)
        & (own_places[:, None] >= offset_all[None, :])
        & (own_places[:, None] < offset_all[None, :] + POOL),
        axis=1,
    )
    start_state = jnp.where(covered[:, None], image_rows, text[0])

    chunk_rows = shard_rows // CHUNKS
    positions = jnp.concatenate(
        [
            (part_at ^ slot) * shard_rows
            + at * chunk_rows
            + jnp.arange(chunk_rows, dtype=jnp.int32)
            for at in range(CHUNKS)
            for slot in slots
        ]
    )
    seg_slots = jnp.concatenate(
        [
            lax.dynamic_slice_in_dim(
                seg_all, (part_at ^ slot) * shard_rows + at * chunk_rows, chunk_rows, 1
            )
            for at in range(CHUNKS)
            for slot in slots
        ],
        axis=1,
    )
    freqs = ROPE_BASE ** (-2.0 * jnp.arange(HD // 2, dtype=jnp.float32) / HD)
    angles = positions.astype(jnp.float32)[:, None] * freqs[None, :]
    cosine, sinus = jnp.cos(angles), jnp.sin(angles)
    query_width = w_query.shape[2]
    w_joined = jnp.concatenate([w_query[0], w_kv[0, 0], w_kv[0, 1]], axis=1)
    cosine, sinus, w_joined, seg_slots, _ = lax.optimization_barrier(
        (cosine, sinus, w_joined, seg_slots, totals)
    )

    starts = [start_state[at * chunk_rows : (at + 1) * chunk_rows] for at in range(CHUNKS)]
    injected = [starts] + [
        [lax.ppermute(piece, "section", [(item, 0)]) for piece in starts]
        for item in range(1, sections)
    ]
    finished = [jnp.zeros_like(piece) for piece in starts]
    entry = section_at == 0
    chunks = starts
    for tick in range(2 * sections - 1):
        if 0 < tick < sections:
            chunks = [jnp.where(entry, new, old) for new, old in zip(injected[tick], chunks)]
        micro_at = jnp.mod(tick - section_at, sections)
        seg_row = lax.dynamic_index_in_dim(seg_slots, micro_at, 0, keepdims=False)
        chunks = decoder_layer(
            chunks,
            seg_row,
            positions,
            cosine,
            sinus,
            attn_gain[0],
            w_joined,
            w_out[0],
            query_width,
        )
        done = tick - (sections - 1)
        first = max(0, done)
        pairs = [(at, at + 1) for at in range(first, min(sections - 1, tick + 1))]
        if done >= 0 and done < sections - 1:
            pairs = pairs + [(sections - 1, done)]
        if pairs:
            moved = [lax.ppermute(piece, "section", pairs) for piece in chunks]
            if done >= 0:
                home = section_at == done
                finished = [jnp.where(home, new, old) for new, old in zip(moved, finished)]
            chunks = moved
    last = section_at == sections - 1
    finished = [jnp.where(last, new, old) for new, old in zip(chunks, finished)]
    return (jnp.concatenate(finished, axis=0)[None], token_weight)


def solution(mesh):
    in_specs = (
        P("section", ("dp", "mp"), None),
        P(("section", "dp"), None),
        P("section", "dp", None),
        P("section", ("dp", "mp")),
        P("dp", None),
        P("dp", None),
        P("section", None),
        P("section", None, "mp"),
        P("section", None, None, "mp"),
        P("section", "mp", None),
        P(),
        P(),
        P(None, ("section", "dp"), "mp"),
        P("mp", ("section", "dp")),
        P(("section", "dp"), "mp"),
        P("mp", ("section", "dp")),
        P(("section", "dp"), "mp"),
    )
    out_specs = (P("section", ("dp", "mp"), None), P("section", ("dp", "mp")))
    return jax.shard_map(shards, mesh=mesh, in_specs=in_specs, out_specs=out_specs, check_vma=False)
```

```python
import jax
import jax.numpy as jnp
from jax import lax
from jax.sharding import PartitionSpec as P

HD = 128
VHD = 64
GRID = 16
PATCH = 256
POOL = 64


EPS = 1e-05
ROPE_BASE = 500000.0
BLOCKED = -1e30


def layer_norm(values, gain, bias):
    wide = values.astype(jnp.float32)
    center = wide - jnp.mean(wide, axis=-1, keepdims=True)
    spread = jnp.mean(center * center, axis=-1, keepdims=True)
    return (center * lax.rsqrt(spread + EPS) * gain + bias).astype(jnp.bfloat16)


def rms_norm(values, gain):
    wide = values.astype(jnp.float32)
    power = jnp.mean(wide * wide, axis=-1, keepdims=True)
    return (wide * lax.rsqrt(power + EPS) * gain).astype(jnp.bfloat16)


def mirrored(value, bit, axis="mp"):
    count = lax.axis_size(axis)
    return lax.ppermute(value, axis, [(at, at ^ bit) for at in range(count)])


def slot_order(count):
    order = [0]
    bit = count // 2
    while bit >= 1:
        order = order + [slot | bit for slot in order]
        bit //= 2
    return order


def gather_slots(piece):
    count = lax.axis_size("mp")
    held = {0: piece}
    bit = count // 2
    while bit >= 1:
        for slot in list(held):
            held[slot | bit] = mirrored(held[slot], bit)
        bit //= 2
    return [held[slot] for slot in slot_order(count)]


def scatter_slots(partial_value, axis="mp"):
    count = lax.axis_size(axis)
    current = partial_value
    bit = 1
    while bit < count:
        half = current.shape[0] // 2
        arrived = mirrored(current[half:].astype(jnp.bfloat16), bit, axis)
        current = current[:half].astype(jnp.float32) + arrived.astype(jnp.float32)
        bit *= 2
    return current


def own_slots(values, part_at, axis="mp"):
    count = lax.axis_size(axis)
    rows = values.shape[0] // count
    return jnp.concatenate(
        [
            lax.dynamic_slice_in_dim(values, (part_at ^ slot) * rows, rows, 0)
            for slot in slot_order(count)
        ],
        axis=0,
    )


def encode_tiles(patches, vis_gain, vis_bias, qkv_full, out_full, up_full, down_full, part_at):
    tile_count = patches.shape[0] // PATCH
    local_width = qkv_full.shape[1] // 3
    head_count = local_width // VHD
    normed = layer_norm(patches, vis_gain[0], vis_bias[0])
    projected = [
        jnp.dot(
            normed,
            qkv_full[:, index * local_width : (index + 1) * local_width],
            preferred_element_type=jnp.float32,
        )
        .astype(jnp.bfloat16)
        .reshape(tile_count, PATCH, head_count, VHD)
        for index in range(3)
    ]
    scores = jnp.einsum(
        "tqhd,tkhd->thqk", projected[0], projected[1], preferred_element_type=jnp.float32
    ) * VHD ** (-0.5)
    probs = jax.nn.softmax(scores, axis=-1).astype(jnp.bfloat16)
    mixed = (
        jnp.einsum("thqk,tkhd->tqhd", probs, projected[2], preferred_element_type=jnp.float32)
        .astype(jnp.bfloat16)
        .reshape(tile_count * PATCH, local_width)
    )
    mixed = own_slots(mixed, part_at)
    attended = scatter_slots(
        jnp.dot(mixed, out_full, preferred_element_type=jnp.float32).astype(jnp.bfloat16)
    )
    rows = attended.shape[0]
    own = lax.dynamic_slice_in_dim(patches, part_at * rows, rows, 0)
    residual = (own.astype(jnp.float32) + attended).astype(jnp.bfloat16)
    normed_two = jnp.concatenate(
        gather_slots(layer_norm(residual, vis_gain[1], vis_bias[1])), axis=0
    )
    inner = jax.nn.gelu(
        jnp.dot(normed_two, up_full, preferred_element_type=jnp.float32), approximate=False
    ).astype(jnp.bfloat16)
    fed = scatter_slots(
        jnp.dot(inner, down_full, preferred_element_type=jnp.float32).astype(jnp.bfloat16)
    )
    states = (residual.astype(jnp.float32) + fed).astype(jnp.bfloat16)
    width = states.shape[1]
    arranged = states.reshape(rows // (2 * GRID), 2, GRID // 2, 2, width)
    return arranged.transpose(0, 2, 1, 3, 4).reshape(rows // 4, 4 * width)


def rotary(joined, cosine, sinus):
    half = HD // 2
    outs = []
    for at in range(0, joined.shape[1], HD):
        first = joined[:, at : at + half]
        second = joined[:, at + half : at + HD]
        outs.append(first * cosine - second * sinus)
        outs.append(second * cosine + first * sinus)
    return jnp.concatenate(outs, axis=1)


CHUNKS = 2


def decoder_layer(chunks, seg_row, positions, cosine, sinus, gain, w_joined, w_out, query_width):
    pair_width = (w_joined.shape[1] - query_width) // 2
    rotated = query_width + pair_width
    pair_heads = pair_width // HD
    group_size = query_width // pair_width
    joined = []
    rows_each = chunks[0].shape[0] * lax.axis_size("mp")
    for at, chunk in enumerate(chunks):
        rows = jnp.concatenate(gather_slots(rms_norm(chunk, gain)), axis=0)
        made = jnp.dot(rows, w_joined, preferred_element_type=jnp.float32)
        part = slice(at * rows_each, (at + 1) * rows_each)
        joined.append(
            jnp.concatenate(
                [rotary(made[:, :rotated], cosine[part], sinus[part]), made[:, rotated:]], axis=1
            ).astype(jnp.bfloat16)
        )
    joined = jnp.concatenate(joined, axis=0)
    length = joined.shape[0]
    query = joined[:, :query_width].reshape(length, pair_heads, group_size, HD)
    keyed = joined[:, query_width:rotated].reshape(length, pair_heads, HD)
    valued = joined[:, rotated:].reshape(length, pair_heads, HD)
    scores = jnp.einsum(
        "qkgd,skd->kgqs", query, keyed, preferred_element_type=jnp.float32
    ) * HD ** (-0.5)
    allowed = (seg_row[:, None] == seg_row[None, :]) & (
        positions[None, :] <= positions[:, None]
    )
    scores = jnp.where(allowed, scores, BLOCKED)
    probs = jax.nn.softmax(scores, axis=-1).astype(jnp.bfloat16)
    mixed = (
        jnp.einsum("kgqs,skd->qkgd", probs, valued, preferred_element_type=jnp.float32)
        .astype(jnp.bfloat16)
        .reshape(length, query_width)
    )
    outs = []
    for at, chunk in enumerate(chunks):
        made = jnp.dot(
            mixed[at * rows_each : (at + 1) * rows_each], w_out, preferred_element_type=jnp.float32
        ).astype(jnp.bfloat16)
        outs.append((chunk.astype(jnp.float32) + scatter_slots(made)).astype(jnp.bfloat16))
    return outs


def shards(
    text,
    patches,
    segments,
    loss_mask,
    tile_batch,
    tile_offset,
    attn_gain,
    w_query,
    w_kv,
    w_out,
    vis_gain,
    vis_bias,
    v_qkv,
    v_out,
    v_up,
    v_down,
    v_proj,
):
    sections = lax.axis_size("section")
    replicas = lax.axis_size("dp")
    parts = lax.axis_size("mp")
    section_at = lax.axis_index("section")
    part_at = lax.axis_index("mp")
    slots = slot_order(parts)
    groups = ("section", "dp")
    qkv_full = lax.all_gather(
        jnp.concatenate([v_qkv[0], v_qkv[1], v_qkv[2]], axis=1), groups, axis=0, tiled=True
    )
    backs = lax.all_gather(
        jnp.concatenate([v_out, v_down], axis=0), groups, axis=1, tiled=True
    )
    up_full = lax.all_gather(v_up, groups, axis=0, tiled=True)
    out_full = backs[: v_out.shape[0]]
    down_full = backs[v_out.shape[0] :]
    length = segments.shape[2]
    totals = lax.psum(lax.psum(lax.psum(jnp.sum(loss_mask), "mp"), "dp"), "section")
    seg_all = lax.all_gather(segments[0, 0], "section", axis=0)
    patches, totals, seg_all = lax.optimization_barrier((patches, totals, seg_all))
    scaling = float(sections * replicas * length)
    token_weight = loss_mask.astype(jnp.float32) * scaling / totals.astype(jnp.float32)

    pooled = encode_tiles(
        patches, vis_gain, vis_bias, qkv_full, out_full, up_full, down_full, part_at
    )
    own_rows = pooled.shape[0]
    group_count = sections * replicas
    depth = v_proj.shape[0]
    cut = pooled.reshape(own_rows, group_count, depth).transpose(1, 0, 2)
    dealt = lax.all_to_all(cut, groups, split_axis=0, concat_axis=0, tiled=True)
    stacked = jnp.stack(gather_slots(dealt), axis=1)
    width = v_proj.shape[1]
    ordered = stacked.reshape(sections, replicas, parts * own_rows, depth).transpose(1, 0, 2, 3)
    projected = jnp.dot(
        own_slots(
            ordered.reshape(group_count * parts * own_rows, depth), lax.axis_index("dp"), "dp"
        ),
        v_proj,
        preferred_element_type=jnp.float32,
    ).astype(jnp.bfloat16)
    image_own = scatter_slots(projected, "dp").astype(jnp.bfloat16)
    image_all = lax.psum(image_own, "section")
    batch_all = tile_batch[0]
    offset_all = tile_offset[0]
    tiles_here = own_rows * parts // POOL
    token_at = jnp.concatenate(
        [(part_at ^ slot) * own_rows + jnp.arange(own_rows, dtype=jnp.int32) for slot in slots]
    )
    tile_at = (
        jnp.arange(sections, dtype=jnp.int32)[:, None] * tiles_here + (token_at // POOL)[None, :]
    ).reshape(-1)
    within = jnp.tile(token_at % POOL, sections)
    tile_ids = jnp.arange(batch_all.shape[0], dtype=jnp.int32)
    pick = (tile_at[:, None] == tile_ids[None, :]).astype(jnp.int32)
    row_batch = jnp.sum(pick * batch_all[None, :], axis=1)
    row_place = jnp.sum(pick * offset_all[None, :], axis=1) + within
    places = jnp.arange(length, dtype=jnp.int32)
    picker = (
        (row_batch == section_at)[None, :] & (places[:, None] == row_place[None, :])
    ).astype(jnp.bfloat16)
    image_cols = jnp.dot(picker, image_all, preferred_element_type=jnp.float32).astype(
        jnp.bfloat16
    )
    image_rows = lax.all_to_all(image_cols, "mp", split_axis=0, concat_axis=1, tiled=True)
    shard_rows = image_rows.shape[0]
    own_places = part_at * shard_rows + jnp.arange(shard_rows, dtype=jnp.int32)
    covered = jnp.any(
        (batch_all[None, :] == section_at)
        & (own_places[:, None] >= offset_all[None, :])
        & (own_places[:, None] < offset_all[None, :] + POOL),
        axis=1,
    )
    start_state = jnp.where(covered[:, None], image_rows, text[0])

    chunk_rows = shard_rows // CHUNKS
    positions = jnp.concatenate(
        [
            (part_at ^ slot) * shard_rows
            + at * chunk_rows
            + jnp.arange(chunk_rows, dtype=jnp.int32)
            for at in range(CHUNKS)
            for slot in slots
        ]
    )
    seg_slots = jnp.concatenate(
        [
            lax.dynamic_slice_in_dim(
                seg_all, (part_at ^ slot) * shard_rows + at * chunk_rows, chunk_rows, 1
            )
            for at in range(CHUNKS)
            for slot in slots
        ],
        axis=1,
    )
    freqs = ROPE_BASE ** (-2.0 * jnp.arange(HD // 2, dtype=jnp.float32) / HD)
    angles = positions.astype(jnp.float32)[:, None] * freqs[None, :]
    cosine, sinus = jnp.cos(angles), jnp.sin(angles)
    query_width = w_query.shape[2]
    w_joined = jnp.concatenate([w_query[0], w_kv[0, 0], w_kv[0, 1]], axis=1)
    cosine, sinus, w_joined, seg_slots, _ = lax.optimization_barrier(
        (cosine, sinus, w_joined, seg_slots, totals)
    )

    starts = [start_state[at * chunk_rows : (at + 1) * chunk_rows] for at in range(CHUNKS)]
    finished = [jnp.zeros_like(piece) for piece in starts]
    entry = section_at == 0
    chunks = starts
    for tick in range(2 * sections - 1):
        if 0 < tick < sections:
            chunks = [jnp.where(entry, new, old) for new, old in zip(injected, chunks)]
        if tick < sections - 1:
            starts, chunks = lax.optimization_barrier((starts, chunks))
            injected = [lax.ppermute(piece, "section", [(tick + 1, 0)]) for piece in starts]
        micro_at = jnp.mod(tick - section_at, sections)
        seg_row = lax.dynamic_index_in_dim(seg_slots, micro_at, 0, keepdims=False)
        chunks = decoder_layer(
            chunks,
            seg_row,
            positions,
            cosine,
            sinus,
            attn_gain[0],
            w_joined,
            w_out[0],
            query_width,
        )
        done = tick - (sections - 1)
        first = max(0, done)
        pairs = [(at, at + 1) for at in range(first, min(sections - 1, tick + 1))]
        if done >= 0 and done < sections - 1:
            pairs = pairs + [(sections - 1, done)]
        if pairs:
            moved = [lax.ppermute(piece, "section", pairs) for piece in chunks]
            if done >= 0:
                home = section_at == done
                finished = [jnp.where(home, new, old) for new, old in zip(moved, finished)]
            chunks = moved
    last = section_at == sections - 1
    finished = [jnp.where(last, new, old) for new, old in zip(chunks, finished)]
    return (jnp.concatenate(finished, axis=0)[None], token_weight)


def solution(mesh):
    in_specs = (
        P("section", ("dp", "mp"), None),
        P(("section", "dp"), None),
        P("section", "dp", None),
        P("section", ("dp", "mp")),
        P("dp", None),
        P("dp", None),
        P("section", None),
        P("section", None, "mp"),
        P("section", None, None, "mp"),
        P("section", "mp", None),
        P(),
        P(),
        P(None, ("section", "dp"), "mp"),
        P("mp", ("section", "dp")),
        P(("section", "dp"), "mp"),
        P("mp", ("section", "dp")),
        P(("section", "dp"), "mp"),
    )
    out_specs = (P("section", ("dp", "mp"), None), P("section", ("dp", "mp")))
    return jax.shard_map(shards, mesh=mesh, in_specs=in_specs, out_specs=out_specs, check_vma=False)
```
